32 devices in a mesh: unit: 4 (over y, core), ep: 4 (over z), fsdp: 2 (over x).
Axes of the slice: x: 2, y: 2, z: 4, core: 2. Of those that a mesh axis runs over, the one named last changes fastest.
Arguments:
- w_down: float32 [256, 1024, 2048], P(('unit', 'ep'), None, 'fsdp'), parts along dimension 0, may hold values from -0.25 to 0.25
- router_weight: float32 [8192, 64], P(('unit', 'fsdp'), 'ep'), parts along dimension 0, may hold values from -0.125 to 0.125
- router_gain: float32 [8192], P(('unit', 'fsdp')), parts along dimension 0, may hold values from 0.25 to 1.75
Outputs:
- serve_down: bfloat16 [256, 1024, 2048], P(('unit', 'ep'), 'fsdp'), parts along dimension 0
- scale_down: float32 [256, 1024], P(('unit', 'ep'), 'fsdp'), parts along dimension 0
- serve_router: bfloat16 [8192, 64], P('unit'), parts along dimension 0
The draws below stay inside these ranges and needn't reach their ends.
There are 4 independent parts, one for each index of `unit`. The reference program is written for one: setup_inputs(seed, part) draws one part's arguments, and reference() takes and returns one part's arrays. A program takes and returns all parts, laid end to end along the dimension named above; each array names one. Nothing has to cross between parts.
All inputs are finite; a program needn't handle non-finite values. Where the reference program divides by a largest or mean magnitude, that divisor is 1e-20 or more.
Results may differ from the reference program's by a relative error of at most 0.001.
Values may be sent and summed in bfloat16 or wider, within the bound.
A program may use at most 256 MiB of HBM per device.

```python
import jax
import jax.numpy as jnp

EXPERTS = 64
D_MODEL = 2048
D_EXPERT = 1024


def spiked(entries, rng, source, target, blocks, factor):
    def block_of(dim):
        return (jnp.arange(entries.shape[dim]) // (entries.shape[dim] // blocks)).reshape((-1,) + (1,) * (entries.ndim - 1 - dim))

    first = jax.random.permutation(rng, blocks)[block_of(target)]
    far = (block_of(target) + blocks // 2) % blocks
    return jnp.where((block_of(source) == first) | (block_of(source) == far), factor * entries, entries)


def block_levels(stream_key, shape, split, least, high):
    level, own = 1.0, jax.random.fold_in(stream_key, 6)
    for axis_at, blocks in split:
        draws = jnp.exp(jax.random.uniform(jax.random.fold_in(own, axis_at), (blocks,), jnp.float32, least / len(split), high / len(split)))
        level = level * jnp.repeat(draws, shape[axis_at] // blocks).reshape([-1 if axis == axis_at else 1 for axis in range(len(shape))])
    return level


def bell_draw(rng, extent, width, most, pieces=(), held_as=jnp.bfloat16):
    loudness = block_levels(rng, extent, pieces, -0.22, 0.18) if pieces else 1.0
    drawn = jax.random.normal(rng, extent, jnp.float32) * width * loudness
    return jnp.minimum(jnp.maximum(drawn, -most), most).astype(held_as)


def bell_draw_with(rng, extent, scale, limit, pieces, heavy, kind=jnp.bfloat16):
    entries = scale * jax.random.normal(rng, extent, jnp.float32)
    if pieces:
        entries = entries * block_levels(rng, extent, pieces, -0.22, 0.18)
    return jnp.clip(spiked(entries, jax.random.fold_in(rng, 3), *heavy), -limit, limit).astype(kind)


def setup_inputs(seed: int = 0, part: int = 0) -> dict:
    splits = jax.random.split(jax.random.key(seed), 4)
    part_keys = jax.random.split(jax.random.fold_in(splits[3], part), 4)
    w_down = bell_draw_with(part_keys[0], (EXPERTS, D_EXPERT, D_MODEL), D_EXPERT ** -0.5, 0.25, ((0, 4), (2, 2)), (2, 1, 2, 2.0), jnp.float32)
    router_weight = bell_draw(part_keys[1], (D_MODEL, EXPERTS), D_MODEL ** -0.5, 0.125, ((0, 2), (1, 4)), jnp.float32)
    router_gain = jnp.clip(1.0 + 0.15 * jax.random.normal(part_keys[2], (D_MODEL,), jnp.float32), 0.25, 1.75)
    return {"w_down": w_down, "router_weight": router_weight, "router_gain": router_gain}


def reference(w_down, router_weight, router_gain):
    scale_down = jnp.sum(jnp.abs(w_down), axis=2) / D_MODEL
    serve_down = (w_down / jnp.expand_dims(scale_down, 2)).astype(jnp.bfloat16)
    serve_router = (router_weight * router_gain[:, None]).astype(jnp.bfloat16)
    return serve_down, scale_down, serve_router
```

```python
import functools

import jax
import jax.numpy as jnp
from jax import lax
from jax.experimental import pallas as pl
from jax.experimental.pallas import tpu as pltpu
from jax.sharding import PartitionSpec as P


LANES = 128
PARAMS = pltpu.CompilerParams(vmem_limit_bytes=67043328)


def cost(read, written):
    return pl.CostEstimate(flops=0, bytes_accessed=read + written, transcendentals=0)


def sums_kernel(place_ref, w_ref, *refs):
    out_ref = refs[-1]
    _, columns = w_ref.shape[1:]
    total = jnp.abs(w_ref[0, :, :LANES])
    for at in range(LANES, columns, LANES):
        total = total + jnp.abs(w_ref[0, :, at : at + LANES])
    out_ref[0] = jnp.sum(total.T, axis=0, keepdims=True)


def sums(place, w, first, count, after, step):
    rows, columns = w.shape[1:]
    step = min(rows, step)
    return pl.pallas_call(
        sums_kernel,
        grid_spec=pltpu.PrefetchScalarGridSpec(
            num_scalar_prefetch=1,
            grid=(count, rows // step),
            in_specs=[pl.BlockSpec((1, step, columns), lambda e, r, p: (first + e, r, 0))]
            + [pl.BlockSpec(memory_space=pl.ANY)] * len(after),
            out_specs=pl.BlockSpec((1, 1, step), lambda e, r, p: (e, 0, r)),
        ),
        out_shape=jax.ShapeDtypeStruct((count, 1, rows), jnp.float32),
        compiler_params=PARAMS,
        cost_estimate=cost(4 * count * rows * columns, 4 * count * rows),
        name="sums",
    )(place, w, *after)


def inverse_column(parts, width):
    total = parts[0][0, 0]
    for part in parts[1:]:
        total = total + part[0, 0]
    inverse = 1.0 / (total * (1.0 / width))
    return jnp.broadcast_to(inverse, (LANES, inverse.shape[1])).T


def scaled(w_ref, inverse, put):
    for at in range(0, w_ref.shape[2], LANES):
        put(at, (w_ref[0, :, at : at + LANES] * inverse).astype(jnp.bfloat16))


def narrow_kernel(n, held, width, place_ref, *refs):
    for s in range(n - 1):
        w_ref, parts = refs[s * (held + 1)], refs[s * (held + 1) + 1 : (s + 1) * (held + 1)]
        out_ref = refs[len(refs) - (n - 1) + s]

        def put(at, value):
            out_ref[0, :, at : at + LANES] = value

        scaled(w_ref, inverse_column(parts, width), put)


def narrow(n, place, w, parts, width, first, count, base, after):
    rows, columns = w.shape[1] // n, w.shape[2]
    parts = [part.reshape(part.shape[0], n, 1, rows) for part in parts]
    in_specs, operands = [], []
    for s in range(1, n):
        in_specs.append(
            pl.BlockSpec((1, rows, columns), lambda e, p, s=s: (first + e, lax.rem(p[0] + s, n), 0))
        )
        in_specs += [
            pl.BlockSpec((1, 1, 1, rows), lambda e, p, s=s: (first - base + e, lax.rem(p[0] + s, n), 0, 0))
        ] * len(parts)
        operands += [w, *parts]
    shape = jax.ShapeDtypeStruct((count, rows, columns), jnp.bfloat16)
    return pl.pallas_call(
        functools.partial(narrow_kernel, n, len(parts), width),
        grid_spec=pltpu.PrefetchScalarGridSpec(
            num_scalar_prefetch=1,
            grid=(count,),
            in_specs=in_specs + [pl.BlockSpec(memory_space=pl.ANY)] * len(after),
            out_specs=[pl.BlockSpec((1, rows, columns), lambda e, p: (e, 0, 0))] * (n - 1),
        ),
        out_shape=[shape] * (n - 1),
        compiler_params=PARAMS,
        cost_estimate=cost(4 * count * (n - 1) * rows * columns, 2 * count * (n - 1) * rows * columns),
        name="narrow",
    )(place, *operands, *after)


def join_kernel(n, held, width, place_ref, w_ref, *refs):
    parts, arrived, out_ref = refs[:held], refs[held : held + n - 1], refs[-1]
    columns = w_ref.shape[2]
    me = place_ref[0]

    def put(at, value):
        out_ref[0, :, pl.ds(pl.multiple_of(me * columns + at, LANES), LANES)] = value

    scaled(w_ref, inverse_column(parts, width), put)
    for s in range(1, n):
        source = lax.rem(me + s, n)
        out_ref[0, :, pl.ds(pl.multiple_of(source * columns, LANES), columns)] = arrived[s - 1][0]


def join(n, place, w, parts, arrived, width, first, count, base, out):
    rows, columns = w.shape[1] // n, w.shape[2]
    parts = [part.reshape(part.shape[0], n, 1, rows) for part in parts]
    in_specs = [pl.BlockSpec((1, rows, columns), lambda e, p: (first + e, p[0], 0))]
    in_specs += [pl.BlockSpec((1, 1, 1, rows), lambda e, p: (first - base + e, p[0], 0, 0))] * len(parts)
    in_specs += [pl.BlockSpec((1, rows, columns), lambda e, p: (e, 0, 0))] * (n - 1)
    operands = [place, w, *parts, *arrived]
    aliases = {}
    if out is not None:
        in_specs.append(pl.BlockSpec(memory_space=pl.ANY))
        aliases = {len(operands): 0}
        operands.append(out)
    return pl.pallas_call(
        functools.partial(join_kernel, n, len(parts), width),
        grid_spec=pltpu.PrefetchScalarGridSpec(
            num_scalar_prefetch=1,
            grid=(count,),
            in_specs=in_specs,
            out_specs=pl.BlockSpec((1, rows, n * columns), lambda e, p: (first + e, 0, 0)),
        ),
        out_shape=jax.ShapeDtypeStruct((w.shape[0], rows, n * columns), jnp.bfloat16),
        input_output_aliases=aliases,
        compiler_params=PARAMS,
        cost_estimate=cost((4 + 2 * (n - 1)) * count * rows * columns, 2 * n * count * rows * columns),
        name="join",
    )(*operands)


def own_kernel(width, place_ref, w_ref, *refs):
    out_ref = refs[-1]

    def put(at, value):
        out_ref[0, :, at : at + LANES] = value

    scaled(w_ref, inverse_column(refs[:-1], width), put)


def own(n, place, w, parts, width, first, count, base):
    rows, columns = w.shape[1] // n, w.shape[2]
    parts = [part.reshape(part.shape[0], n, 1, rows) for part in parts]
    return pl.pallas_call(
        functools.partial(own_kernel, width),
        grid_spec=pltpu.PrefetchScalarGridSpec(
            num_scalar_prefetch=1,
            grid=(count,),
            in_specs=[pl.BlockSpec((1, rows, columns), lambda e, p: (first + e, p[0], 0))]
            + [pl.BlockSpec((1, 1, 1, rows), lambda e, p: (first - base + e, p[0], 0, 0))] * len(parts),
            out_specs=pl.BlockSpec((1, rows, columns), lambda e, p: (first + e, 0, p[0])),
        ),
        out_shape=jax.ShapeDtypeStruct((w.shape[0], rows, n * columns), jnp.bfloat16),
        compiler_params=PARAMS,
        cost_estimate=cost(4 * count * rows * columns, 2 * count * rows * columns),
        name="own",
    )(place, w, *parts)


def lay_kernel(place_ref, block_ref, *refs):
    refs[-1][...] = block_ref[...]


def lay(n, place, arrived, s, first, out, after):
    count, rows, columns = arrived.shape
    return pl.pallas_call(
        lay_kernel,
        grid_spec=pltpu.PrefetchScalarGridSpec(
            num_scalar_prefetch=1,
            grid=(count,),
            in_specs=[pl.BlockSpec((1, rows, columns), lambda e, p: (e, 0, 0))]
            + [pl.BlockSpec(memory_space=pl.ANY)] * (1 + len(after)),
            out_specs=pl.BlockSpec((1, rows, columns), lambda e, p: (first + e, 0, lax.rem(p[0] + s, n))),
        ),
        out_shape=jax.ShapeDtypeStruct(out.shape, out.dtype),
        input_output_aliases={2: 0},
        compiler_params=PARAMS,
        cost_estimate=cost(2 * count * rows * columns, 2 * count * rows * columns),
        name="lay",
    )(place, arrived, out, *after)


def settle_kernel(router_ref, out_ref):
    out_ref[...] = router_ref[...]


def settle(router):
    return pl.pallas_call(
        settle_kernel,
        out_shape=jax.ShapeDtypeStruct(router.shape, router.dtype),
        compiler_params=PARAMS,
        cost_estimate=cost(2 * router.size, 2 * router.size),
        name="settle",
    )(router)


def exchange(value_of, n):
    got = [None] * n
    for s in range(1, n):
        got[n - s] = lax.ppermute(value_of(s), "fsdp", [(i, (i + s) % n) for i in range(n)])
    return got[1:]


def plan_of(experts):
    if experts < 8:
        return [1] * experts, [experts]
    middle = experts - 4
    thirds = [middle // 3 + (i < middle % 3) for i in range(3)]
    return [1, 1, 1] + thirds + [1], [1, 2, 4]


def swapped(n, part):
    got = exchange(lambda s: part, n)
    return [part] + got if n <= 2 else [sum(got, part)]


def on_device(n, w_down, router_weight, router_gain):
    return steps(n, w_down, router_weight, router_gain)


def steps(n, w_down, router_weight, router_gain):
    experts, rows, columns = w_down.shape
    width = n * columns
    me = lax.axis_index("fsdp")
    place = jnp.reshape(me, (1,)).astype(jnp.int32)

    chunks, groups = plan_of(experts)
    firsts = [sum(chunks[:at]) for at in range(len(chunks))]
    parts_of, sent, arrived = [], [], []
    totals = []

    def group(at):
        begin = sum(groups[:at])
        base, count = firsts[begin], sum(chunks[begin : begin + groups[at]])
        after = tuple(sent[-1]) if at == 2 else (totals[0],) if at == 1 else ()
        part = sums(place, w_down, base, count, after, 512 if at == 0 else 1024)
        totals.append(part)
        parts_of.extend([(base, swapped(n, part))] * groups[at])

    group(0)
    if len(groups) > 1:
        group(1)
    for at, count in enumerate(chunks):
        if at == 2 and len(groups) > 2:
            group(2)
        base, parts = parts_of[at]
        after = tuple(sent[-1]) if sent else ()
        if at == 2:
            after += (totals[-1],)
        out = narrow(n, place, w_down, parts, width, firsts[at], count, base, after)
        sent.append(out)
        arrived.append(exchange(lambda s: out[s - 1], n))

    if n > 1:
        router_weight, _ = lax.optimization_barrier((router_weight, sent[0][0]))
    part_router = (router_weight.T * router_gain[None, :]).astype(jnp.bfloat16)
    routers = [part_router] + exchange(lambda s: part_router, n)
    slots = []
    for source in range(n):
        piece = routers[0]
        for s in range(1, n):
            piece = jnp.where((me + s) % n == source, routers[s], piece)
        slots.append(piece)
    row_router = jnp.concatenate(slots, axis=1)
    if n > 1:
        row_router, _ = lax.optimization_barrier((row_router, sent[-1][0]))
    serve_router = settle(lax.all_gather(row_router, "ep", axis=0, tiled=True))

    last = len(chunks) - 1
    base, parts = parts_of[last]
    serve_down = own(n, place, w_down, parts, width, firsts[last], chunks[last], base)
    for at in range(last):
        base, parts = parts_of[at]
        serve_down = join(n, place, w_down, parts, arrived[at], width, firsts[at], chunks[at], base, serve_down)
    for s in range(1, n):
        serve_down = lay(n, place, arrived[last][s - 1], s, firsts[last], serve_down, (serve_router,))

    whole, seen = [], 0
    for size in groups:
        parts = parts_of[seen][1]
        whole.append(sum(parts[1:], parts[0]))
        seen += size
    scale_down = jnp.concatenate(whole, axis=0)[:, 0] / width
    scale_down = lax.dynamic_slice_in_dim(scale_down, me * (rows // n), rows // n, axis=1)
    return (serve_down, scale_down, serve_router.T)


def solution(mesh):
    n = mesh.shape["fsdp"]

    def whole(w_down, router_weight, router_gain):
        step = jax.shard_map(
            functools.partial(on_device, n),
            mesh=mesh,
            in_specs=(P(("unit", "ep"), None, "fsdp"), P(("unit", "fsdp"), "ep"), P(("unit", "fsdp"))),
            out_specs=(P(("unit", "ep"), "fsdp", None), P(("unit", "ep"), "fsdp"), P("unit", None)),
            check_vma=False,
        )
        return step(w_down, router_weight, router_gain)

    return whole
```
